32 devices in a mesh: section: 1, ep: 32 (over z, y, x, core).
Axes of the slice: x: 2, y: 2, z: 4, core: 2. Of those that a mesh axis runs over, the one named last changes fastest.
Arguments:
- saved_inputs: bfloat16 [1, 4096, 4096], P('section', 'ep'), may hold values from -6 to 6
- expert_ids: int32 [1, 4096, 2], P('section', 'ep'), may hold values from 0 to 7, as said below
- gate_weights: float32 [1, 4096, 2], P('section', 'ep'), may hold values from 0.1 to 0.9
- out_grad: bfloat16 [4096, 4096], P('ep', 'section'), may hold values from -6 to 6
- gate_w: bfloat16 [1, 7168, 4096], P('section', 'ep'), may hold values from -0.09375 to 0.09375
- up_w: bfloat16 [1, 7168, 4096], P('section', 'ep'), may hold values from -0.09375 to 0.09375
- down_w: bfloat16 [1, 7168, 4096], P('section', 'ep'), may hold values from -0.0625 to 0.0625
Outputs:
- input_grads: bfloat16 [1, 4096, 4096], P('section', 'ep')
- grad_gate: bfloat16 [1, 7168, 4096], P('section', 'ep')
- grad_up: bfloat16 [1, 7168, 4096], P('section', 'ep')
- grad_down: bfloat16 [1, 7168, 4096], P('section', 'ep')
The draws below stay inside these ranges and needn't reach their ends.
Inputs may be any that keep to these rules, and one draw needn't show every extreme that they name: `expert_ids`: the two ids of a token differ. Among the 128 tokens of one device in one layer, at most 4 name expert 0, and in every layer some device's tokens name it exactly 4 times.
All inputs are finite; a program needn't handle non-finite values.
Results may differ from the reference program's by a relative error of at most 0.0058.
Values may be sent and summed in bfloat16 or wider, within the bound.
A program may use at most 128 MiB of HBM per device.

```python
import jax
import jax.numpy as jnp
from jax import lax

D = 4096
EXPERTS = 8
TOK_DEV = 128
CAP = 4
FFW = 7168
SECTIONS = 1
TOKENS = 4096
N_EP = 32


def draw_expert_ids(key, part):
    groups = TOKENS // TOK_DEV
    blocks = SECTIONS * groups
    keys = jax.random.split(key, 7)
    first_count = jax.random.randint(keys[0], (SECTIONS, groups), 1, CAP + 1)
    second_count = jax.random.randint(keys[1], (SECTIONS, groups), 1, CAP + 1)
    counts = jnp.minimum(first_count, second_count)
    fullest = jax.random.randint(keys[2], (SECTIONS, 1), 0, groups)
    counts = jnp.where(jnp.arange(groups)[None, :] == fullest, CAP, counts).reshape(blocks, 1)
    ranks = jax.vmap(lambda block_key: jax.random.permutation(block_key, TOK_DEV))(jax.random.split(keys[3], blocks))
    is_live = ranks < counts
    other_first = jax.random.randint(keys[4], (blocks, TOK_DEV), 1, EXPERTS)
    other_second = jax.random.randint(keys[5], (blocks, TOK_DEV), 1, EXPERTS - 1)
    other_second = other_second + (other_second >= other_first).astype(jnp.int32)
    which_side = jax.random.randint(keys[6], (blocks, TOK_DEV), 0, 2)
    id_zero = jnp.where(is_live, jnp.where(which_side == 0, 0, other_first), other_first)
    id_one = jnp.where(is_live, jnp.where(which_side == 0, other_first, 0), other_second)
    return jnp.stack([id_zero, id_one], -1).reshape(SECTIONS, TOKENS, 2).astype(jnp.int32)


def steps_of(key, shape, cuts, least, top_value):
    level, own = 1.0, jax.random.fold_in(key, 6)
    for dim, blocks in cuts:
        draws = jnp.exp(jax.random.uniform(jax.random.fold_in(own, dim), (blocks,), jnp.float32, least / len(cuts), top_value / len(cuts)))
        level = level * jnp.repeat(draws, shape[dim] // blocks).reshape([-1 if axis == dim else 1 for axis in range(len(shape))])
    return level


def gaussian(own_key, extent, scale, limit, cuts=(), held_as=jnp.bfloat16):
    values = scale * jax.random.normal(own_key, extent, jnp.float32)
    if cuts:
        values = values * steps_of(own_key, extent, cuts, -0.22, 0.18)
    return jnp.clip(values, -limit, limit).astype(held_as)


def setup_inputs(seed: int = 0) -> dict:
    key_list = jax.random.split(jax.random.key(seed), 8)
    return {
        "saved_inputs": gaussian(key_list[0], (SECTIONS, TOKENS, D), 1.0, 6.0, ((1, 32),)),
        "expert_ids": draw_expert_ids(jax.random.fold_in(key_list[7], 71), 0),
        "gate_weights": jnp.clip(0.1 + 0.79999997 * jax.random.uniform(key_list[2], (SECTIONS, TOKENS, 2), jnp.float32) ** steps_of(key_list[2], (SECTIONS, TOKENS, 2), ((1, 32),), -0.2, 0.2), 0.1, 0.9),
        "out_grad": gaussian(key_list[3], (TOKENS, D), 1.0, 6.0, ((0, 32),)),
        "gate_w": gaussian(key_list[4], (SECTIONS, FFW, D), D ** -0.5, 0.09375, ((1, 32),)),
        "up_w": gaussian(key_list[5], (SECTIONS, FFW, D), D ** -0.5, 0.09375, ((1, 32),)),
        "down_w": gaussian(key_list[6], (SECTIONS, FFW, D), FFW ** -0.5, 0.0625, ((1, 32),)),
    }


def reference(saved_inputs, expert_ids, gate_weights, out_grad, gate_w, up_w, down_w):
    device_of = (jnp.arange(TOKENS, dtype=jnp.int32) // TOK_DEV).astype(jnp.int32)

    def section_backward(upstream, operands):
        tokens, routes, gate_share, w_gate, w_up, w_down = operands
        is_live = routes == 0
        live_count = jnp.sum(is_live.astype(jnp.int32), axis=1).astype(jnp.int32)
        pair_weight = jnp.sum(jnp.where(is_live, gate_share, 0.0), axis=1)
        per_device = live_count.reshape(N_EP, TOK_DEV)
        slot_index = (jnp.cumsum(per_device, axis=1) - per_device).reshape(TOKENS).astype(jnp.int32)
        target = (device_of * (CAP + 1) + jnp.where(live_count == 1, slot_index, CAP)).astype(jnp.int32)

        def pack_rows(row_data):
            buffer = jnp.zeros((N_EP * (CAP + 1), D), row_data.dtype).at[target].set(row_data)
            return buffer.reshape(N_EP, CAP + 1, D)[:, :CAP].reshape(N_EP * CAP, D)

        scaled = (pair_weight[:, None] * upstream.astype(jnp.float32)).astype(jnp.bfloat16)
        x_rows = pack_rows(tokens)
        y_rows = pack_rows(scaled)
        gate_pre = jnp.dot(x_rows, w_gate.T, preferred_element_type=jnp.float32)
        up_pre = jnp.dot(x_rows, w_up.T, preferred_element_type=jnp.float32)
        sigmoid_gate = jax.nn.sigmoid(gate_pre)
        activated = gate_pre * sigmoid_gate
        hidden = (activated * up_pre).astype(jnp.bfloat16)
        grad_hidden = jnp.dot(y_rows, w_down.T, preferred_element_type=jnp.float32)
        d_up = (grad_hidden * activated).astype(jnp.bfloat16)
        d_gate = (grad_hidden * up_pre * sigmoid_gate * (1.0 + gate_pre * (1.0 - sigmoid_gate))).astype(jnp.bfloat16)
        back_rows = (jnp.dot(d_gate, w_gate, preferred_element_type=jnp.float32)
                     + jnp.dot(d_up, w_up, preferred_element_type=jnp.float32))
        padded = jnp.concatenate([back_rows.reshape(N_EP, CAP, D),
                                  jnp.zeros((N_EP, 1, D), back_rows.dtype)], 1).reshape(N_EP * (CAP + 1), D)
        input_grad = (upstream.astype(jnp.float32) + padded[target]).astype(jnp.bfloat16)
        grad_gate = jnp.dot(d_gate.T, x_rows, preferred_element_type=jnp.float32).astype(jnp.bfloat16)
        grad_up = jnp.dot(d_up.T, x_rows, preferred_element_type=jnp.float32).astype(jnp.bfloat16)
        grad_down = jnp.dot(hidden.T, y_rows, preferred_element_type=jnp.float32).astype(jnp.bfloat16)
        return input_grad, (input_grad, grad_gate, grad_up, grad_down)

    final_grad, outputs = lax.scan(section_backward, out_grad,
                                   (saved_inputs, expert_ids, gate_weights, gate_w, up_w, down_w), reverse=True)
    return (outputs[0], outputs[1], outputs[2], outputs[3])
```

```python
import functools

import jax
import jax.numpy as jnp
from jax import lax
from jax.experimental import pallas as pl
from jax.experimental.pallas import tpu as pltpu
from jax.sharding import PartitionSpec as P

CAP = 4
PAIR = 2 * CAP
CHUNKS = 2
MESH = pl.DeviceIdType.MESH
F32 = jnp.float32
BF16 = jnp.bfloat16


def from_behind(value, axis, by):
    devices = lax.axis_size(axis)
    pairs = [(i, i + by) for i in range(devices) if 0 <= i + by < devices]
    return lax.ppermute(value, axis, pairs)


def exchange_kernel(
    depth, routes_ref, share_ref, tokens_hbm, current_hbm, wg_hbm, wu_hbm, wd_hbm,
    back_ref, select_ref, dg_ref, du_ref, hidden_ref, x_hbm, y_hbm,
    tok, wg, wu, wd, packed, pair_in, zbuf, full, pre,
    psend, prem, pown, qsend, qrecv, hsend, hrecv, total, zsend, zrecv, back,
    load_sem, pair_send, pair_recv, z_send, z_recv, p_send, p_recv, q_send, q_recv, d_send, d_recv,
    out_sem, rd_send, rd_recv, rq_send, rq_recv, rp_send, rp_recv, rz_send, rz_recv, rb_send, rb_recv,
):
    me = lax.axis_index("ep")
    c = me % 2
    a = (me // 2) % 2
    b = (me // 4) % 2
    z = me // 8
    own = b * 2 + a
    flip_a = 1 - 2 * a
    flip_b = 2 - 4 * b
    step_p = (1 - c) * flip_a + c * flip_b
    step_q = c * flip_a + (1 - c) * flip_b
    near_p, near_q, near_pq = own + step_p, own + step_q, own + step_p + step_q
    mate = me + 1 - 2 * c
    dev_p, dev_q = me + 2 * step_p, me + 2 * step_q
    other = 1 - c

    def dev_z(d):
        return (z + d) % depth * 8 + me % 8

    half = full.shape[-1]
    rows = full.shape[-2]
    chunk = half // CHUNKS

    def remote(src, dst, send_sem, recv_sem, device):
        return pltpu.make_async_remote_copy(
            src_ref=src, dst_ref=dst, send_sem=send_sem, recv_sem=recv_sem,
            device_id={"ep": device}, device_id_type=MESH,
        )

    loads = [
        pltpu.make_async_copy(src, dst, load_sem.at[i])
        for i, (src, dst) in enumerate(
            [(tokens_hbm, tok.at[0]), (current_hbm, tok.at[1]), (wg_hbm, wg), (wu_hbm, wu), (wd_hbm, wd)]
        )
    ]
    for load in loads:
        load.start()

    barrier = pltpu.get_barrier_semaphore()
    peers = [mate, dev_p, dev_q] + [dev_z(d) for d in range(1, depth)]
    for peer in peers:
        pl.semaphore_signal(barrier, inc=1, device_id={"ep": peer}, device_id_type=MESH)

    live = (routes_ref[0:1, :] == 0) | (routes_ref[1:2, :] == 0)
    weight = jnp.where(routes_ref[0:1, :] == 0, share_ref[0:1, :], 0.0) + jnp.where(
        routes_ref[1:2, :] == 0, share_ref[1:2, :], 0.0
    )
    count = live.shape[1]
    live_f = live.astype(F32)
    before = (
        lax.broadcasted_iota(jnp.int32, (count, count), 0) < lax.broadcasted_iota(jnp.int32, (count, count), 1)
    ).astype(F32)
    slot = jnp.dot(
        jnp.broadcast_to(live_f, (PAIR, count)).astype(BF16), before.astype(BF16), preferred_element_type=F32
    )
    place = lax.broadcasted_iota(jnp.int32, (PAIR, count), 0) - c * CAP
    chosen = (
        (slot == place.astype(F32)) & (place >= 0) & (place < CAP) & (jnp.broadcast_to(live_f, (PAIR, count)) > 0.5)
    )
    select = chosen.astype(F32)
    select_ref[...] = select
    slot_weight = jnp.sum(select * weight, axis=1, keepdims=True)
    selector = select.astype(BF16)

    pl.semaphore_wait(barrier, len(peers))

    pair_copies = []
    for m in range(2):
        loads[m].wait()
        for h in range(2):
            picked = jnp.dot(selector, tok[m, :, h * half : (h + 1) * half], preferred_element_type=F32)
            if m == 1:
                picked = picked * slot_weight
            packed[m, h] = picked.astype(BF16)
        copy = remote(packed.at[m, other], pair_in.at[m], pair_send.at[m], pair_recv.at[m], mate)
        copy.start()
        pair_copies.append(copy)

    sent = list(pair_copies)
    z_copies = [[], []]
    for m in range(2):
        pair_copies[m].wait_recv()
        zbuf[m, z] = (packed[m, c].astype(F32) + pair_in[m].astype(F32)).astype(BF16)
        for d in range(1, depth):
            copy = remote(zbuf.at[m, z], zbuf.at[m, z], z_send.at[m, d], z_recv.at[m, d], dev_z(d))
            copy.start()
            z_copies[m].append(copy)
            sent.append(copy)

    p_copies, q_copies, d_copies = [None, None], [[], []], [[], []]

    def group(m, g):
        return full.at[m, c, g]

    def to_mate(m, i, g):
        copy = remote(group(m, g), group(m, g), d_send.at[m, i], d_recv.at[m, i], mate)
        copy.start()
        d_copies[m].append(copy)
        sent.append(copy)

    def to_q(m, i, g):
        copy = remote(group(m, g), group(m, g), q_send.at[m, i], q_recv.at[m, i], dev_q)
        copy.start()
        q_copies[m].append(copy)
        sent.append(copy)

    for m in range(2):
        for copy in z_copies[m]:
            copy.wait_recv()
        full[m, c, own] = jnp.concatenate([zbuf[m, i].astype(F32) for i in range(depth)], axis=0).astype(BF16)
        p_copies[m] = remote(group(m, own), group(m, own), p_send.at[m], p_recv.at[m], dev_p)
        p_copies[m].start()
        sent.append(p_copies[m])
        to_q(m, 0, own)
        to_mate(m, 0, own)
    for m in range(2):
        p_copies[m].wait_recv()
        to_q(m, 1, near_p)
        to_mate(m, 1, near_p)

    def finish(m):
        q_copies[m][0].wait_recv()
        to_mate(m, 2, near_q)
        q_copies[m][1].wait_recv()
        to_mate(m, 3, near_pq)

    def arrive(m):
        for copy in d_copies[m]:
            copy.wait_recv()

    tile = 512
    tiles = half // tile

    def project(weights, m):
        def body(t, value):
            for h in range(2):
                start = pl.multiple_of(t * tile, tile)
                data = full[m, h, :, :, pl.ds(start, tile)].reshape(4 * rows, tile)
                value = value + lax.dot_general(
                    weights[:, pl.ds(pl.multiple_of(h * half + t * tile, tile), tile)], data,
                    (((1,), (1,)), ((), ())), preferred_element_type=F32,
                )
            return value

        return lax.fori_loop(0, tiles, body, jnp.zeros((weights.shape[0], 4 * rows), F32))

    finish(0)
    arrive(0)
    loads[2].wait()
    pre[0] = project(wg, 0)
    finish(1)
    loads[3].wait()
    pre[1] = project(wu, 0)
    loads[4].wait()
    arrive(1)
    outs = [
        pltpu.make_async_copy(full.at[0], x_hbm, out_sem.at[0]),
        pltpu.make_async_copy(full.at[1], y_hbm, out_sem.at[1]),
    ]
    for out in outs:
        out.start()
    grad_hidden = project(wd, 1)
    gate_pre, up_pre = pre[0], pre[1]
    sig = jax.nn.sigmoid(gate_pre)
    act = gate_pre * sig
    hidden_ref[...] = (act * up_pre).astype(BF16)
    du_ref[...] = (grad_hidden * act).astype(BF16)
    dg_ref[...] = (grad_hidden * up_pre * sig * (1.0 + gate_pre * (1.0 - sig))).astype(BF16)

    wide = min(512, chunk)

    def contract(h, k, store):
        def body(t, carry):
            inner = pl.multiple_of(t * wide, wide)
            start = pl.multiple_of(h * half + k * chunk + t * wide, wide)
            dims = (((0,), (0,)), ((), ()))
            part = lax.dot_general(dg_ref[...], wg[:, pl.ds(start, wide)], dims, preferred_element_type=F32)
            part += lax.dot_general(du_ref[...], wu[:, pl.ds(start, wide)], dims, preferred_element_type=F32)
            store(pl.ds(inner, wide), part.reshape(4, rows, wide))
            return carry

        lax.fori_loop(0, chunk // wide, body, 0)

    rd, rq, rp, rz, rb = [], [], [], [], []
    for k in range(CHUNKS):
        def store_send(cols, part, k=k):
            psend[k, :, :, cols] = part.astype(BF16)

        contract(other, k, store_send)
        copy = remote(psend.at[k], prem.at[k], rd_send.at[k], rd_recv.at[k], mate)
        copy.start()
        rd.append(copy)
    for k in range(CHUNKS):
        def store_own(cols, part, k=k):
            pown[k, :, :, cols] = part

        contract(c, k, store_own)
    for k in range(CHUNKS):
        rd[k].wait_recv()
        pair = []
        for i, g in enumerate((near_pq, near_q)):
            qsend[k, i] = (pown[k, g] + prem[k, g].astype(F32)).astype(BF16)
            copy = remote(qsend.at[k, i], qrecv.at[k, i], rq_send.at[k, i], rq_recv.at[k, i], dev_q)
            copy.start()
            pair.append(copy)
        rq.append(pair)
    for k in range(CHUNKS):
        rq[k][0].wait_recv()
        hsend[k] = (pown[k, near_p] + prem[k, near_p].astype(F32) + qrecv[k, 0].astype(F32)).astype(BF16)
        copy = remote(hsend.at[k], hrecv.at[k], rp_send.at[k], rp_recv.at[k], dev_p)
        copy.start()
        rp.append(copy)
    for k in range(CHUNKS):
        rq[k][1].wait_recv()
        mine = pown[k, own] + prem[k, own].astype(F32) + qrecv[k, 1].astype(F32)
        rp[k].wait_recv()
        total[k] = (mine + hrecv[k].astype(F32)).reshape(depth, PAIR, chunk)
        some = []
        for d in range(1, depth):
            zsend[k, d] = total[k, (z + d) % depth].astype(BF16)
            copy = remote(zsend.at[k, d], zrecv.at[k, d], rz_send.at[k, d], rz_recv.at[k, d], dev_z(d))
            copy.start()
            some.append(copy)
        rz.append(some)
    for k in range(CHUNKS):
        value = total[k, z]
        for d in range(1, depth):
            rz[k][d - 1].wait_recv()
            value = value + zrecv[k, d].astype(F32)
        back[c, k] = value
        copy = remote(back.at[c, k], back.at[c, k], rb_send.at[k], rb_recv.at[k], mate)
        copy.start()
        rb.append(copy)
    for k in range(CHUNKS):
        rb[k].wait_recv()
    back_ref[...] = back[...]
    for copy in sent + rd + rp + rb + sum(rq, []) + sum(rz, []):
        copy.wait_send()
    for out in outs:
        out.wait()


def exchange(routes, shares, tokens, current, w_gate, w_up, w_down, devices):
    depth = devices // 8
    count, width = tokens.shape
    units = w_gate.shape[0]
    half = width // 2
    chunk = half // CHUNKS
    rows = depth * PAIR
    slots = devices * CAP
    dma = pltpu.SemaphoreType.DMA
    vmem = pl.BlockSpec(memory_space=pltpu.VMEM)
    hbm = pl.BlockSpec(memory_space=pl.ANY)
    return pl.pallas_call(
        functools.partial(exchange_kernel, depth),
        out_shape=(
            jax.ShapeDtypeStruct((2, CHUNKS, PAIR, chunk), F32),
            jax.ShapeDtypeStruct((PAIR, count), F32),
            jax.ShapeDtypeStruct((units, slots), BF16),
            jax.ShapeDtypeStruct((units, slots), BF16),
            jax.ShapeDtypeStruct((units, slots), BF16),
            jax.ShapeDtypeStruct((2, 4, rows, half), BF16),
            jax.ShapeDtypeStruct((2, 4, rows, half), BF16),
        ),
        in_specs=[vmem, vmem] + [hbm] * 5,
        out_specs=(vmem,) * 5 + (hbm,) * 2,
        scratch_shapes=[
            pltpu.VMEM((2, count, width), BF16),
            pltpu.VMEM((units, width), BF16),
            pltpu.VMEM((units, width), BF16),
            pltpu.VMEM((units, width), BF16),
            pltpu.VMEM((2, 2, PAIR, half), BF16),
            pltpu.VMEM((2, PAIR, half), BF16),
            pltpu.VMEM((2, depth, PAIR, half), BF16),
            pltpu.VMEM((2, 2, 4, rows, half), BF16),
            pltpu.VMEM((2, units, slots), F32),
            pltpu.VMEM((CHUNKS, 4, rows, chunk), BF16),
            pltpu.VMEM((CHUNKS, 4, rows, chunk), BF16),
            pltpu.VMEM((CHUNKS, 4, rows, chunk), F32),
            pltpu.VMEM((CHUNKS, 2, rows, chunk), BF16),
            pltpu.VMEM((CHUNKS, 2, rows, chunk), BF16),
            pltpu.VMEM((CHUNKS, rows, chunk), BF16),
            pltpu.VMEM((CHUNKS, rows, chunk), BF16),
            pltpu.VMEM((CHUNKS, depth, PAIR, chunk), F32),
            pltpu.VMEM((CHUNKS, depth, PAIR, chunk), BF16),
            pltpu.VMEM((CHUNKS, depth, PAIR, chunk), BF16),
            pltpu.VMEM((2, CHUNKS, PAIR, chunk), F32),
            dma((5,)), dma((2,)), dma((2,)), dma((2, depth)), dma((2, depth)), dma((2,)), dma((2,)),
            dma((2, 2)), dma((2, 2)), dma((2, 4)), dma((2, 4)), dma((2,)),
            dma((CHUNKS,)), dma((CHUNKS,)), dma((CHUNKS, 2)), dma((CHUNKS, 2)),
            dma((CHUNKS,)), dma((CHUNKS,)), dma((CHUNKS, depth)), dma((CHUNKS, depth)),
            dma((CHUNKS,)), dma((CHUNKS,)),
        ],
        compiler_params=pltpu.CompilerParams(
            collective_id=0, has_side_effects=True, vmem_limit_bytes=56 * 1024 * 1024
        ),
        name="exchange",
    )(routes, shares, tokens, current, w_gate, w_up, w_down)


def outputs_kernel(back_ref, select_ref, dg_ref, du_ref, hidden_ref, x_ref, y_ref, current_ref,
                   input_ref, gate_ref, up_ref, down_ref):
    slots = dg_ref.shape[1]
    x_rows = x_ref[0].reshape(slots, x_ref.shape[-1])
    y_rows = y_ref[0].reshape(slots, y_ref.shape[-1])
    gate_ref[...] = jnp.dot(dg_ref[...], x_rows, preferred_element_type=F32).astype(BF16)
    up_ref[...] = jnp.dot(du_ref[...], x_rows, preferred_element_type=F32).astype(BF16)
    down_ref[...] = jnp.dot(hidden_ref[...], y_rows, preferred_element_type=F32).astype(BF16)
    spread = lax.dot_general(
        select_ref[...], back_ref[0, 0], (((0,), (0,)), ((), ())),
        preferred_element_type=F32, precision=lax.Precision.HIGHEST,
    )
    input_ref[...] = (current_ref[...].astype(F32) + spread).astype(BF16)


def outputs(back, select, d_gate, d_up, hidden, x_rows, y_rows, current):
    count, width = current.shape
    units, slots = d_gate.shape
    half = width // 2
    tile = 512
    per_half = half // tile
    per_chunk = back.shape[-1] // tile
    whole = lambda t: (0, 0)
    columns = lambda t: (0, t)
    data = pl.BlockSpec((1,) + x_rows.shape[1:3] + (tile,), lambda t: (t // per_half, 0, 0, t % per_half))
    return pl.pallas_call(
        outputs_kernel,
        grid=(width // tile,),
        out_shape=(
            jax.ShapeDtypeStruct((count, width), BF16),
            jax.ShapeDtypeStruct((units, width), BF16),
            jax.ShapeDtypeStruct((units, width), BF16),
            jax.ShapeDtypeStruct((units, width), BF16),
        ),
        in_specs=[
            pl.BlockSpec(
                (1, 1, PAIR, tile),
                lambda t: (t // per_half, t % per_half // per_chunk, 0, t % per_chunk),
            ),
            pl.BlockSpec((PAIR, count), whole),
            pl.BlockSpec((units, slots), whole),
            pl.BlockSpec((units, slots), whole),
            pl.BlockSpec((units, slots), whole),
            data,
            data,
            pl.BlockSpec((count, tile), columns),
        ],
        out_specs=(
            pl.BlockSpec((count, tile), columns),
            pl.BlockSpec((units, tile), columns),
            pl.BlockSpec((units, tile), columns),
            pl.BlockSpec((units, tile), columns),
        ),
        name="outputs",
    )(back, select, d_gate, d_up, hidden, x_rows, y_rows, current)


def on_device(saved_inputs, expert_ids, gate_weights, out_grad, gate_w, up_w, down_w):
    sections = lax.axis_size("section")
    section_index = lax.axis_index("section")
    devices = lax.axis_size("ep")
    routes = expert_ids[0].T
    shares = gate_weights[0].T
    current = out_grad if sections == 1 else lax.all_gather(out_grad, "section", axis=1, tiled=True)
    kept = None
    for step_index in range(sections):
        active = section_index == sections - 1 - step_index
        parts = exchange(routes, shares, saved_inputs[0], current, gate_w[0], up_w[0], down_w[0], devices)
        made = outputs(*parts, current)
        kept = made if kept is None else tuple(jnp.where(active, new, old) for new, old in zip(made, kept))
        if step_index + 1 < sections:
            current = from_behind(made[0], "section", -1)
    return tuple(value[None] for value in kept)


def solution(mesh):
    placed = (
        P("section", "ep", None),
        P("section", "ep", None),
        P("section", "ep", None),
        P("ep", "section"),
        P("section", "ep", None),
        P("section", "ep", None),
        P("section", "ep", None),
    )
    return jax.shard_map(
        on_device,
        mesh=mesh,
        in_specs=placed,
        out_specs=(
            P("section", "ep", None),
            P("section", "ep", None),
            P("section", "ep", None),
            P("section", "ep", None),
        ),
        check_vma=False,
    )
```

```python
import functools

import jax
import jax.numpy as jnp
from jax import lax
from jax.experimental import pallas as pl
from jax.experimental.pallas import tpu as pltpu
from jax.sharding import PartitionSpec as P

CAP = 4
CHUNKS = 2
MESH = pl.DeviceIdType.MESH
F32 = jnp.float32
BF16 = jnp.bfloat16


def from_behind(value, axis, by):
    devices = lax.axis_size(axis)
    pairs = [(i, i + by) for i in range(devices) if 0 <= i + by < devices]
    return lax.ppermute(value, axis, pairs)


def exchange_kernel(
    depth, routes_hbm, share_hbm, tokens_hbm, current_hbm, wg_hbm, wu_hbm, wd_hbm,
    back_ref, select_ref, gate_ref, up_ref, down_ref,
    routes_ref, share_ref, dg_ref, du_ref, hidden_ref, tok, wg, wu, wd, packed, zbuf, full, pre,
    psend, prem, pown, qsend, qrecv, hsend, hrecv, total, zsend, zrecv,
    load_sem, z_send, z_recv, p_send, p_recv, q_send, q_recv, d_send, d_recv,
    rd_send, rd_recv, rq_send, rq_recv, rp_send, rp_recv, rz_send, rz_recv,
):
    me = lax.axis_index("ep")
    c = me % 2
    a = (me // 2) % 2
    b = (me // 4) % 2
    z = me // 8
    own = b * 2 + a
    flip_a = 1 - 2 * a
    flip_b = 2 - 4 * b
    step_p = (1 - c) * flip_a + c * flip_b
    step_q = c * flip_a + (1 - c) * flip_b
    near_p, near_q, near_pq = own + step_p, own + step_q, own + step_p + step_q
    mate = me + 1 - 2 * c
    dev_p, dev_q = me + 2 * step_p, me + 2 * step_q
    other = 1 - c

    def dev_z(d, core):
        return (z + d) % depth * 8 + own * 2 + core

    half = full.shape[-1]
    rows = full.shape[-2]
    chunk = half // CHUNKS

    def remote(src, dst, send_sem, recv_sem, device):
        return pltpu.make_async_remote_copy(
            src_ref=src, dst_ref=dst, send_sem=send_sem, recv_sem=recv_sem,
            device_id={"ep": device}, device_id_type=MESH,
        )

    loads = [
        pltpu.make_async_copy(src, dst, load_sem.at[i])
        for i, (src, dst) in enumerate(
            [
                (tokens_hbm, tok.at[0]), (current_hbm, tok.at[1]), (wg_hbm, wg), (wu_hbm, wu), (wd_hbm, wd),
                (routes_hbm, routes_ref), (share_hbm, share_ref),
            ]
        )
    ]
    for load in loads[5:] + loads[:5]:
        load.start()

    barrier = pltpu.get_barrier_semaphore()
    peers = [mate, dev_p, dev_q] + [dev_z(d, h) for d in range(1, depth) for h in range(2)]
    for peer in peers:
        pl.semaphore_signal(barrier, inc=1, device_id={"ep": peer}, device_id_type=MESH)

    loads[5].wait()
    loads[6].wait()
    live = (routes_ref[0:1, :] == 0) | (routes_ref[1:2, :] == 0)
    weight = jnp.where(routes_ref[0:1, :] == 0, share_ref[0:1, :], 0.0) + jnp.where(
        routes_ref[1:2, :] == 0, share_ref[1:2, :], 0.0
    )
    count = live.shape[1]
    live_f = live.astype(F32)
    before = (
        lax.broadcasted_iota(jnp.int32, (count, count), 0) < lax.broadcasted_iota(jnp.int32, (count, count), 1)
    ).astype(F32)
    slot = jnp.dot(
        jnp.broadcast_to(live_f, (CAP, count)).astype(BF16), before.astype(BF16), preferred_element_type=F32
    )
    place = lax.broadcasted_iota(jnp.int32, (CAP, count), 0)
    chosen = (
        (slot == place.astype(F32)) & (jnp.broadcast_to(live_f, (CAP, count)) > 0.5)
    )
    select = chosen.astype(F32)
    select_ref[...] = select
    slot_weight = jnp.sum(select * weight, axis=1, keepdims=True)
    selector = select.astype(BF16)

    pl.semaphore_wait(barrier, len(peers))

    sent = []
    z_copies = [[], []]
    for m in range(2):
        loads[m].wait()
        for h in range(2):
            picked = jnp.dot(selector, tok[m, :, h * half : (h + 1) * half], preferred_element_type=F32)
            if m == 1:
                picked = picked * slot_weight
            packed[m, h] = picked.astype(BF16)
        for d in range(1, depth):
            for h in range(2):
                z_copies[m].append(
                    remote(packed.at[m, h], zbuf.at[m, z, c], z_send.at[m, d, h], z_recv.at[m, d, c], dev_z(d, h))
                )
        z_copies[m].append(
            remote(packed.at[m, other], zbuf.at[m, z, c], z_send.at[m, 0, 0], z_recv.at[m, 0, 0], mate)
        )
        for copy in z_copies[m]:
            copy.start()
        sent += z_copies[m]
        zbuf[m, z, c] = packed[m, c]

    def from_z(m):
        for d in range(1, depth):
            for h in range(2):
                remote(packed.at[m, h], zbuf.at[m, z, c], z_send.at[m, d, h], z_recv.at[m, d, h], mate).wait_recv()
        z_copies[m][-1].wait_recv()

    p_copies, q_copies, d_copies = [None, None], [[], []], [[], []]

    def group(m, g):
        return full.at[m, c, g]

    def to_mate(m, i, g):
        copy = remote(group(m, g), group(m, g), d_send.at[m, i], d_recv.at[m, i], mate)
        copy.start()
        d_copies[m].append(copy)
        sent.append(copy)

    def to_q(m, i, g):
        copy = remote(group(m, g), group(m, g), q_send.at[m, i], q_recv.at[m, i], dev_q)
        copy.start()
        q_copies[m].append(copy)
        sent.append(copy)

    for m in range(2):
        from_z(m)
        full[m, c, own] = jnp.concatenate(
            [zbuf[m, i, h].astype(F32) for i in range(depth) for h in range(2)], axis=0
        ).astype(BF16)
        p_copies[m] = remote(group(m, own), group(m, own), p_send.at[m], p_recv.at[m], dev_p)
        p_copies[m].start()
        sent.append(p_copies[m])
        to_q(m, 0, own)
        to_mate(m, 0, own)
    for m in range(2):
        p_copies[m].wait_recv()
        to_q(m, 1, near_p)
        to_mate(m, 1, near_p)

    def finish(m):
        q_copies[m][0].wait_recv()
        to_mate(m, 2, near_q)
        q_copies[m][1].wait_recv()
        to_mate(m, 3, near_pq)

    def arrive(m):
        for copy in d_copies[m]:
            copy.wait_recv()

    tile = 512
    tiles = half // tile

    def project(weights, m, h, value):
        def body(t, value):
            start = pl.multiple_of(t * tile, tile)
            data = full[m, h, :, :, pl.ds(start, tile)].reshape(4 * rows, tile)
            return value + lax.dot_general(
                weights[:, pl.ds(pl.multiple_of(h * half + t * tile, tile), tile)], data,
                (((1,), (1,)), ((), ())), preferred_element_type=F32,
            )

        return lax.fori_loop(0, tiles, body, value)

    def weight_grad(out_ref, left_ref, m):
        left = left_ref[...]
        for h in range(2):
            def body(t, carry):
                data = full[m, h, :, :, pl.ds(pl.multiple_of(t * tile, tile), tile)].reshape(4 * rows, tile)
                cols = pl.ds(pl.multiple_of(h * half + t * tile, tile), tile)
                out_ref[:, cols] = jnp.dot(left, data, preferred_element_type=F32).astype(BF16)
                return carry

            lax.fori_loop(0, tiles, body, 0)

    zero = jnp.zeros((wg.shape[0], 4 * rows), F32)
    finish(0)
    loads[2].wait()
    pre[0] = project(wg, 0, c, zero)
    arrive(0)
    pre[0] = project(wg, 0, other, pre[0])
    loads[3].wait()
    pre[1] = project(wu, 0, c, zero)
    finish(1)
    loads[4].wait()
    pre[1] = project(wu, 0, other, pre[1])
    grad_hidden = project(wd, 1, c, zero)
    arrive(1)
    grad_hidden = project(wd, 1, other, grad_hidden)
    gate_pre, up_pre = pre[0], pre[1]
    sig = jax.nn.sigmoid(gate_pre)
    act = gate_pre * sig
    hidden_ref[...] = (act * up_pre).astype(BF16)
    du_ref[...] = (grad_hidden * act).astype(BF16)
    dg_ref[...] = (grad_hidden * up_pre * sig * (1.0 + gate_pre * (1.0 - sig))).astype(BF16)

    wide = min(512, chunk)

    def contract(h, k, store):
        def body(t, carry):
            inner = pl.multiple_of(t * wide, wide)
            start = pl.multiple_of(h * half + k * chunk + t * wide, wide)
            dims = (((0,), (0,)), ((), ()))
            part = lax.dot_general(dg_ref[...], wg[:, pl.ds(start, wide)], dims, preferred_element_type=F32)
            part += lax.dot_general(du_ref[...], wu[:, pl.ds(start, wide)], dims, preferred_element_type=F32)
            store(pl.ds(inner, wide), part.reshape(4, rows, wide))
            return carry

        lax.fori_loop(0, chunk // wide, body, 0)

    rd, rq, rp, rz = [], [], [], []
    for k in range(CHUNKS):
        def store_send(cols, part, k=k):
            psend[k, :, :, cols] = part.astype(BF16)

        contract(other, k, store_send)
        copy = remote(psend.at[k], prem.at[k], rd_send.at[k], rd_recv.at[k], mate)
        copy.start()
        rd.append(copy)
    for k in range(CHUNKS):
        def store_own(cols, part, k=k):
            pown[k, :, :, cols] = part

        contract(c, k, store_own)
    for k in range(CHUNKS):
        rd[k].wait_recv()
        pair = []
        for i, g in enumerate((near_pq, near_q)):
            qsend[k, i] = (pown[k, g] + prem[k, g].astype(F32)).astype(BF16)
            copy = remote(qsend.at[k, i], qrecv.at[k, i], rq_send.at[k, i], rq_recv.at[k, i], dev_q)
            copy.start()
            pair.append(copy)
        rq.append(pair)
    weight_grad(gate_ref, dg_ref, 0)
    for k in range(CHUNKS):
        rq[k][0].wait_recv()
        hsend[k] = (pown[k, near_p] + prem[k, near_p].astype(F32) + qrecv[k, 0].astype(F32)).astype(BF16)
        copy = remote(hsend.at[k], hrecv.at[k], rp_send.at[k], rp_recv.at[k], dev_p)
        copy.start()
        rp.append(copy)
    weight_grad(up_ref, du_ref, 0)
    for k in range(CHUNKS):
        rq[k][1].wait_recv()
        mine = pown[k, own] + prem[k, own].astype(F32) + qrecv[k, 1].astype(F32)
        rp[k].wait_recv()
        mine = mine + hrecv[k].astype(F32)
        for i in range(depth):
            for h in range(2):
                start = (2 * i + h) * CAP
                total[k, i, h] = mine[start : start + CAP]
        some = []
        for d in range(1, depth):
            for h in range(2):
                zsend[k, d, h] = total[k, (z + d) % depth, h].astype(BF16)
                some.append(
                    remote(zsend.at[k, d, h], zrecv.at[k, d, c], rz_send.at[k, d, h], rz_recv.at[k, d, c], dev_z(d, h))
                )
                some[-1].start()
        zsend[k, 0, 0] = total[k, z, other].astype(BF16)
        some.append(remote(zsend.at[k, 0, 0], zrecv.at[k, 0, c], rz_send.at[k, 0, 0], rz_recv.at[k, 0, 0], mate))
        some[-1].start()
        rz.append(some)
    weight_grad(down_ref, hidden_ref, 1)
    for k in range(CHUNKS):
        for d in range(1, depth):
            for h in range(2):
                remote(
                    zsend.at[k, d, h], zrecv.at[k, d, h], rz_send.at[k, d, h], rz_recv.at[k, d, h], mate
                ).wait_recv()
        rz[k][-1].wait_recv()
        back_ref[c, k] = total[k, z, c] + sum(zrecv[k, d, c].astype(F32) for d in range(1, depth))
        back_ref[other, k] = sum(zrecv[k, d, other].astype(F32) for d in range(depth))
    for copy in sent + rd + rp + sum(rq, []) + sum(rz, []):
        copy.wait_send()


def exchange(routes, shares, tokens, current, w_gate, w_up, w_down, devices):
    depth = devices // 8
    count, width = tokens.shape
    units = w_gate.shape[0]
    operands = (routes, shares, tokens, current, w_gate, w_up, w_down)
    half = width // 2
    chunk = half // CHUNKS
    rows = depth * 2 * CAP
    slots = devices * CAP
    dma = pltpu.SemaphoreType.DMA
    vmem = pl.BlockSpec(memory_space=pltpu.VMEM)
    hbm = pl.BlockSpec(memory_space=pltpu.HBM)
    return pl.pallas_call(
        functools.partial(exchange_kernel, depth),
        out_shape=(
            jax.ShapeDtypeStruct((2, CHUNKS, CAP, chunk), F32),
            jax.ShapeDtypeStruct((CAP, count), F32),
            jax.ShapeDtypeStruct((units, width), BF16),
            jax.ShapeDtypeStruct((units, width), BF16),
            jax.ShapeDtypeStruct((units, width), BF16),
        ),
        in_specs=[hbm] * 7,
        out_specs=(vmem,) * 5,
        scratch_shapes=[
            pltpu.VMEM(routes.shape, jnp.int32),
            pltpu.VMEM(shares.shape, F32),
            pltpu.VMEM((units, slots), BF16),
            pltpu.VMEM((units, slots), BF16),
            pltpu.VMEM((units, slots), BF16),
            pltpu.VMEM((2, count, width), BF16),
            pltpu.VMEM((units, width), BF16),
            pltpu.VMEM((units, width), BF16),
            pltpu.VMEM((units, width), BF16),
            pltpu.VMEM((2, 2, CAP, half), BF16),
            pltpu.VMEM((2, depth, 2, CAP, half), BF16),
            pltpu.VMEM((2, 2, 4, rows, half), BF16),
            pltpu.VMEM((2, units, slots), F32),
            pltpu.VMEM((CHUNKS, 4, rows, chunk), BF16),
            pltpu.VMEM((CHUNKS, 4, rows, chunk), BF16),
            pltpu.VMEM((CHUNKS, 4, rows, chunk), F32),
            pltpu.VMEM((CHUNKS, 2, rows, chunk), BF16),
            pltpu.VMEM((CHUNKS, 2, rows, chunk), BF16),
            pltpu.VMEM((CHUNKS, rows, chunk), BF16),
            pltpu.VMEM((CHUNKS, rows, chunk), BF16),
            pltpu.VMEM((CHUNKS, depth, 2, CAP, chunk), F32),
            pltpu.VMEM((CHUNKS, depth, 2, CAP, chunk), BF16),
            pltpu.VMEM((CHUNKS, depth, 2, CAP, chunk), BF16),
            dma((7,)), dma((2, depth, 2)), dma((2, depth, 2)), dma((2,)), dma((2,)),
            dma((2, 2)), dma((2, 2)), dma((2, 4)), dma((2, 4)),
            dma((CHUNKS,)), dma((CHUNKS,)), dma((CHUNKS, 2)), dma((CHUNKS, 2)),
            dma((CHUNKS,)), dma((CHUNKS,)), dma((CHUNKS, depth, 2)), dma((CHUNKS, depth, 2)),
        ],
        compiler_params=pltpu.CompilerParams(
            collective_id=0, has_side_effects=True, vmem_limit_bytes=28 * 1024 * 1024
        ),
        name="exchange",
    )(*[pltpu.with_memory_space_constraint(v, pltpu.HBM) for v in operands])


def outputs_kernel(back_ref, select_ref, gate_ref, up_ref, down_ref, current_hbm,
                   input_hbm, gate_hbm, up_hbm, down_hbm, held, made, load_sem, store_sem):
    parts = 2 * CHUNKS
    tile = held.shape[1] // parts
    loads, stores = [], []
    for i in range(parts):
        cols = pl.ds(i * tile, tile)
        loads.append(pltpu.make_async_copy(current_hbm.at[:, cols], held.at[:, cols], load_sem.at[i]))
        loads[-1].start()
    for i, (src, dst) in enumerate([(gate_ref, gate_hbm), (up_ref, up_hbm), (down_ref, down_hbm)]):
        stores.append(pltpu.make_async_copy(src, dst, store_sem.at[i]))
        stores[-1].start()
    for i in range(parts):
        cols = pl.ds(i * tile, tile)
        spread = lax.dot_general(
            select_ref[...], back_ref[i // CHUNKS, i % CHUNKS], (((0,), (0,)), ((), ())),
            preferred_element_type=F32, precision=lax.Precision.HIGHEST,
        )
        loads[i].wait()
        made[:, cols] = (held[:, cols].astype(F32) + spread).astype(BF16)
        stores.append(pltpu.make_async_copy(made.at[:, cols], input_hbm.at[:, cols], store_sem.at[3 + i]))
        stores[-1].start()
    for store in stores:
        store.wait()


def outputs(back, select, grad_gate, grad_up, grad_down, current):
    vmem = pl.BlockSpec(memory_space=pltpu.VMEM)
    hbm = pl.BlockSpec(memory_space=pltpu.HBM)
    shape = jax.ShapeDtypeStruct(grad_gate.shape, BF16)
    return pl.pallas_call(
        outputs_kernel,
        out_shape=(jax.ShapeDtypeStruct(current.shape, BF16), shape, shape, shape),
        in_specs=[vmem] * 5 + [hbm],
        out_specs=(hbm,) * 4,
        scratch_shapes=[
            pltpu.VMEM(current.shape, BF16),
            pltpu.VMEM(current.shape, BF16),
            pltpu.SemaphoreType.DMA((2 * CHUNKS,)),
            pltpu.SemaphoreType.DMA((3 + 2 * CHUNKS,)),
        ],
        compiler_params=pltpu.CompilerParams(vmem_limit_bytes=16 * 1024 * 1024),
        name="outputs",
    )(back, select, grad_gate, grad_up, grad_down, current)


def on_device(saved_inputs, expert_ids, gate_weights, out_grad, gate_w, up_w, down_w):
    sections = lax.axis_size("section")
    section_index = lax.axis_index("section")
    devices = lax.axis_size("ep")
    routes = expert_ids[0].T
    shares = gate_weights[0].T
    current = out_grad if sections == 1 else lax.all_gather(out_grad, "section", axis=1, tiled=True)
    kept = None
    for step_index in range(sections):
        active = section_index == sections - 1 - step_index
        parts = exchange(routes, shares, saved_inputs[0], current, gate_w[0], up_w[0], down_w[0], devices)
        made = outputs(*parts, current)
        kept = made if kept is None else tuple(jnp.where(active, new, old) for new, old in zip(made, kept))
        if step_index + 1 < sections:
            current = from_behind(made[0], "section", -1)
    return tuple(value[None] for value in kept)


def solution(mesh):
    placed = (
        P("section", "ep", None),
        P("section", "ep", None),
        P("section", "ep", None),
        P("ep", "section"),
        P("section", "ep", None),
        P("section", "ep", None),
        P("section", "ep", None),
    )
    return jax.shard_map(
        on_device,
        mesh=mesh,
        in_specs=placed,
        out_specs=(
            P("section", "ep", None),
            P("section", "ep", None),
            P("section", "ep", None),
            P("section", "ep", None),
        ),
        check_vma=False,
    )
```
